32 devices in a mesh: expert: 8 (over z, x), shard: 4 (over y, core).
Axes of the slice: x: 2, y: 2, z: 4, core: 2. Of those that a mesh axis runs over, the one named last changes fastest.
Arguments:
- train_down: float32 [16, 6400, 4096], P('expert', None, 'shard'), may hold values from -0.109375 to 0.109375
- router_weight: float32 [4096, 16], P('shard', 'expert'), may hold values from -0.09375 to 0.09375
- router_gain: float32 [4096], P('shard'), may hold values from 0.25 to 1.75
Outputs:
- ready_down: bfloat16 [16, 6400, 4096], P('expert', 'shard')
- scale_down: float32 [16, 6400], P('expert', 'shard')
- serve_router: bfloat16 [4096, 16], replicated
The draws below stay inside these ranges and needn't reach their ends.
All inputs are finite; a program needn't handle non-finite values. Where the reference program divides by a largest or mean magnitude, that divisor is 1e-20 or more.
Results may differ from the reference program's by a relative error of at most 0.001.
Values may be sent and summed in bfloat16 or wider, within the bound.
A program may use at most 192 MiB of HBM per device.

```python
import jax
import jax.numpy as jnp

EXPERTS = 16
D_MODEL = 4096
D_EXPERT = 6400


def raised(drawn, rng, source, target, parts, factor):
    def block_of(position):
        return (jnp.arange(drawn.shape[position]) // (drawn.shape[position] // parts)).reshape((-1,) + (1,) * (drawn.ndim - 1 - position))

    first = jax.random.permutation(rng, parts)[block_of(target)]
    other_side = (block_of(target) + parts // 2) % parts
    return jnp.where((block_of(source) == first) | (block_of(source) == other_side), factor * drawn, drawn)


def level_of(rng, shape, pieces, least, high):
    factor_of, own = 1.0, jax.random.fold_in(rng, 6)
    for dim, parts in pieces:
        heights = jnp.exp(jax.random.uniform(jax.random.fold_in(own, dim), (parts,), jnp.float32, least / len(pieces), high / len(pieces)))
        factor_of = factor_of * jnp.repeat(heights, shape[dim] // parts).reshape([-1 if axis == dim else 1 for axis in range(len(shape))])
    return factor_of


def normal_values(key, shape, width, bound, split=(), held_as=jnp.bfloat16):
    result = width * jax.random.normal(key, shape, jnp.float32)
    if split:
        result = result * level_of(key, shape, split, -0.22, 0.18)
    return jnp.clip(result, -bound, bound).astype(held_as)


def noise_with(key, dims, spread, most, cuts, heavy, kind=jnp.bfloat16):
    result = spread * jax.random.normal(key, dims, jnp.float32)
    if cuts:
        result = result * level_of(key, dims, cuts, -0.22, 0.18)
    return jnp.clip(raised(result, jax.random.fold_in(key, 3), *heavy), -most, most).astype(kind)


def setup_inputs(seed: int = 0) -> dict:
    streams_of = jax.random.split(jax.random.key(seed), 4)
    train_down = noise_with(streams_of[0], (EXPERTS, D_EXPERT, D_MODEL), D_EXPERT ** -0.5, 0.109375, ((0, 8), (2, 4)), (2, 1, 4, 2.0), jnp.float32)
    router_weight = normal_values(streams_of[1], (D_MODEL, EXPERTS), D_MODEL ** -0.5, 0.09375, ((0, 4), (1, 8)), jnp.float32)
    router_gain = jnp.clip(1.0 + 0.15 * jax.random.normal(streams_of[2], (D_MODEL,), jnp.float32), 0.25, 1.75)
    return dict(train_down=train_down, router_weight=router_weight, router_gain=router_gain)


def reference(train_down, router_weight, router_gain):
    scale_down = jnp.max(jnp.abs(train_down), axis=2)
    ready_down = (train_down / jnp.expand_dims(scale_down, 2)).astype(jnp.bfloat16)
    serve_router = (router_weight * router_gain[:, None]).astype(jnp.bfloat16)
    return ready_down, scale_down, serve_router
```

```python
import functools

import jax
import jax.numpy as jnp
from jax import lax
from jax.experimental import pallas as pl
from jax.experimental.pallas import tpu as pltpu
from jax.sharding import PartitionSpec as P

LANES = 128
LEAD = 16
HEAD = 4
AHEAD = 6
HOLD = 5
DEFER = 6
TAIL_PART = 10
PLACE_ROWS = 160
RING = 16
MESH = pl.DeviceIdType.MESH


def rows_per_step(count, n):
    fits = [r for r in range(16, count + 1, 16) if count % r == 0]
    return [r for r in fits if (n * r) % LANES == 0][0]


def swap(i, k):
    for b in range(k.bit_length()):
        if (k >> b) & 1:
            i = i + (1 << b) * (1 - 2 * ((i // (1 << b)) % 2))
    return i


def exchange_kernel(n, ne, rows, done, parts, lead, head, x_hbm, weight_ref, gain_ref, *rest):
    far = range(2, n)
    main_hbm = rest[0]
    tails = [rest[1 + p * len(far) : 1 + (p + 1) * len(far)] for p in range(len(parts))]
    rest = rest[1 + len(parts) * len(far) :]
    scale_ref, router_ref = rest[:2]
    (xbuf, narrow, own_max, seen_max, load_sem, max_send, max_recv,
     data_send, data_recv, keep_sem, router_send, router_recv) = rest[2:]
    experts, all_rows, width = x_hbm.shape
    count = all_rows // n
    blocks = count // rows
    steps = experts * blocks
    slots = xbuf.shape[0]
    groups = n * rows // LANES
    me = lax.axis_index("shard")
    mine = lax.axis_index("expert")
    late = me % 2
    bits = [1 << b for b in range(ne.bit_length() - 1)]

    def load(i, t):
        e, b = i // blocks, i % blocks
        return pltpu.make_async_copy(
            x_hbm.at[e, pl.ds(t * count + b * rows, rows), :],
            xbuf.at[i % slots, pl.ds(t * rows, rows), :],
            load_sem.at[i % slots],
        )

    def start_load(i):
        for t in range(n):
            load(i, t).start()

    for i in range(min(AHEAD, steps)):
        start_load(i)

    barrier = pltpu.get_barrier_semaphore()
    for k in range(1, n):
        pl.semaphore_signal(barrier, inc=1, device_id={"shard": swap(me, k)}, device_id_type=MESH)
    for bit in bits:
        pl.semaphore_signal(barrier, inc=1, device_id={"expert": swap(mine, bit)}, device_id_type=MESH)

    router_ref[mine, me] = (weight_ref[...] * gain_ref[...]).astype(jnp.bfloat16)

    def local_max(i):
        @pl.when(i + AHEAD < steps)
        def _():
            start_load(i + AHEAD)

        slot = i % slots
        pltpu.make_async_copy(xbuf.at[slot], xbuf.at[slot], load_sem.at[slot]).wait()
        for g in range(groups):
            at = pl.ds(g * LANES, LANES)
            top = jnp.abs(xbuf[slot, at, 0:LANES])
            for c in range(LANES, width, LANES):
                top = jnp.maximum(top, jnp.abs(xbuf[slot, at, c : c + LANES]))
            own_max[i, :, at] = jnp.max(top.T, axis=0, keepdims=True)

    def send_max(i):
        for k in range(1, n):
            pltpu.make_async_remote_copy(
                src_ref=own_max.at[i],
                dst_ref=seen_max.at[i, k - 1],
                send_sem=max_send.at[0],
                recv_sem=max_recv.at[i],
                device_id={"shard": swap(me, k)},
                device_id_type=MESH,
            ).start()

    def divide(j):
        slot = j % slots
        pltpu.make_async_copy(seen_max.at[j], seen_max.at[j], max_recv.at[j]).wait()
        full = own_max[j]
        for k in range(1, n):
            full = jnp.maximum(full, seen_max[j, k - 1])
        scale_ref[j] = full
        for g in range(groups):
            at = pl.ds(g * LANES, LANES)
            column = jnp.broadcast_to(full[:, g * LANES : (g + 1) * LANES], (LANES, LANES)).T
            for c in range(0, width, LANES):
                narrow[j, at, c : c + LANES] = (xbuf[slot, at, c : c + LANES] / column).astype(jnp.bfloat16)

    def block_of(j, k):
        return narrow.at[j, pl.ds(pl.multiple_of(swap(me, k) * rows, rows), rows), :]

    def spot(j, k):
        return main_hbm.at[k, pl.ds(pl.multiple_of(j * rows, rows), rows), :]

    def push(j, k):
        pltpu.make_async_remote_copy(
            src_ref=block_of(j, k),
            dst_ref=spot(j, k),
            send_sem=data_send.at[k],
            recv_sem=data_recv.at[k],
            device_id={"shard": swap(me, k)},
            device_id_type=MESH,
        ).start()

    def push_far(j):
        for k in reversed(far):
            i = j - late * (HOLD if k % 2 else HOLD + DEFER)

            @pl.when((i >= 0) & (i < done))
            def _():
                push(i, k)

    def dispatch(j):
        push_far(j)
        if n > 1:
            push(j, 1)
        pltpu.make_async_copy(block_of(j, 0), spot(j, 0), keep_sem.at[0]).start()
        for p, (first, size) in enumerate(parts):
            @pl.when((j >= first) & (j < first + size))
            def _():
                for k in far:
                    pltpu.make_async_copy(block_of(j, k), tails[p][k - 2].at[j - first], keep_sem.at[1 + p]).start()

    def opening(j, carry):
        local_max(head + 2 * j)
        local_max(head + 2 * j + 1)
        divide(j)
        send_max(head + 2 * j)
        send_max(head + 2 * j + 1)
        dispatch(j)
        return carry

    def steady(j, carry):
        @pl.when(j + lead < steps)
        def _():
            local_max(j + lead)

        divide(j)

        @pl.when(j + lead < steps)
        def _():
            send_max(j + lead)

        dispatch(j)
        return carry

    for i in range(head):
        local_max(i)
    pl.semaphore_wait(barrier, n - 1 + len(bits))
    for i in range(head):
        send_max(i)
    for k in range(1, n):
        pltpu.make_async_remote_copy(
            src_ref=router_ref.at[mine, me], dst_ref=router_ref.at[mine, me],
            send_sem=router_send.at[0], recv_sem=router_recv.at[0],
            device_id={"shard": swap(me, k)}, device_id_type=MESH,
        ).start()
    lax.fori_loop(0, lead - head, opening, 0)

    pieces = router_ref.at[mine, 0 : n - 1]
    pltpu.make_async_copy(pieces, pieces, router_send.at[0]).wait()
    pltpu.make_async_copy(pieces, pieces, router_recv.at[0]).wait()
    for b, bit in enumerate(bits):
        held = router_ref.at[pl.ds(mine - mine % bit, bit)]
        pltpu.make_async_remote_copy(
            src_ref=held, dst_ref=held,
            send_sem=router_send.at[1 + b], recv_sem=router_recv.at[1 + b],
            device_id={"expert": swap(mine, bit)}, device_id_type=MESH,
        ).start()
        pltpu.make_async_copy(held, held, router_send.at[1 + b]).wait()
        pltpu.make_async_copy(held, held, router_recv.at[1 + b]).wait()

    lax.fori_loop(lead - head, steps, steady, 0)
    for j in range(steps, done + HOLD + DEFER):
        push_far(j)

    for _ in range(1, n):
        pltpu.make_async_copy(own_max, own_max, max_send.at[0]).wait()
    for p in range(len(parts)):
        for k in far:
            pltpu.make_async_copy(tails[p][k - 2], tails[p][k - 2], keep_sem.at[1 + p]).wait()
    every = narrow.at[0:steps, 0:rows, :]
    sent = narrow.at[0:done, 0:rows, :]
    pltpu.make_async_copy(every, every, keep_sem.at[0]).wait()
    for k in range(1, n):
        moved = sent if k in far else every
        pltpu.make_async_copy(moved, moved, data_send.at[k]).wait()
        pltpu.make_async_copy(moved, moved, data_recv.at[k]).wait()


def place_kernel(n, cut, tall, main_hbm, out_hbm, ring, load_sem, store_sem):
    total, width = main_hbm.shape[1:]
    me = lax.axis_index("shard")
    near = min(2, n)
    first = n * (cut // tall)
    chunks = first + near * ((total - cut) // tall)
    slots = ring.shape[0]
    behind = slots // 2

    def where(t):
        early = t < first
        u = t - first
        k = jnp.where(early, t % n, u % near)
        row = jnp.where(early, (t // n) * tall, cut + (u // near) * tall)
        source = 0
        for q in range(n):
            source = jnp.where(k == q, swap(me, q), source)
        return k, pl.multiple_of(row, tall), pl.multiple_of(source * width, LANES)

    def load(t):
        k, row, _ = where(t)
        return pltpu.make_async_copy(main_hbm.at[k, pl.ds(row, tall), :], ring.at[t % slots], load_sem.at[t % slots])

    def store(t):
        _, row, column = where(t)
        return pltpu.make_async_copy(
            ring.at[t % slots], out_hbm.at[pl.ds(row, tall), pl.ds(column, width)], store_sem.at[t % slots]
        )

    def step(t, carry):
        @pl.when((t >= slots) & (t < chunks + slots))
        def _():
            store(t - slots).wait()

        @pl.when(t < chunks)
        def _():
            load(t).start()

        @pl.when((t >= behind) & (t < chunks + behind))
        def _():
            load(t - behind).wait()
            store(t - behind).start()

        return carry

    lax.fori_loop(0, chunks + slots, step, 0)


def finish_kernel(n, row, *refs):
    count = n - 2
    parts, out_hbm, sem = refs[:count], refs[-2], refs[-1]
    me = lax.axis_index("shard")
    size, width = parts[0].shape

    def store(k):
        column = pl.multiple_of(swap(me, k) * width, LANES)
        return pltpu.make_async_copy(
            parts[k - 2], out_hbm.at[pl.ds(row, size), pl.ds(column, width)], sem.at[k - 2]
        )

    for k in range(2, n):
        store(k).start()
    for k in range(2, n):
        store(k).wait()


def per_device(n, ne, train_down, router_weight, router_gain):
    experts, all_rows, width = train_down.shape
    count = all_rows // n
    rows = rows_per_step(count, n)
    steps = experts * (count // rows)
    total = steps * rows
    lead = min(LEAD, steps // 2)
    head = min(HEAD, lead - 1)
    tail = max(2, steps // TAIL_PART)
    done = steps - tail
    last = max(1, tail // 5)
    parts = [(done, tail - last), (steps - last, last)]
    far = range(2, n)
    depth, columns = router_weight.shape
    rounds = ne.bit_length()
    bf16, f32 = jnp.bfloat16, jnp.float32
    hbm = pl.BlockSpec(memory_space=pl.ANY)
    vmem = pl.BlockSpec(memory_space=pltpu.VMEM)
    dma = pltpu.SemaphoreType.DMA
    results = pl.pallas_call(
        functools.partial(exchange_kernel, n, ne, rows, done, parts, lead, head),
        out_shape=[jax.ShapeDtypeStruct((n, total, width), bf16)]
        + [jax.ShapeDtypeStruct((size, rows, width), bf16) for _, size in parts for _ in far]
        + [
            jax.ShapeDtypeStruct((steps, 1, n * rows), f32),
            jax.ShapeDtypeStruct((ne, n, columns, depth), bf16),
        ],
        in_specs=[hbm, vmem, vmem],
        out_specs=[hbm] * (1 + len(parts) * len(far)) + [vmem, vmem],
        scratch_shapes=[
            pltpu.VMEM((lead + AHEAD + 1, n * rows, width), f32),
            pltpu.VMEM((steps, n * rows, width), bf16),
            pltpu.VMEM((steps, 1, n * rows), f32),
            pltpu.VMEM((steps, n - 1, 1, n * rows), f32),
            dma((lead + AHEAD + 1,)),
            dma((1,)),
            dma((steps,)),
            dma((n,)),
            dma((n,)),
            dma((1 + len(parts),)),
            dma((rounds,)),
            dma((rounds,)),
        ],
        compiler_params=pltpu.CompilerParams(
            collective_id=0, has_side_effects=True, vmem_limit_bytes=60 * 1024 * 1024
        ),
        name="exchange",
    )(train_down, router_weight.T, router_gain[None, :])
    main, scales, router = results[0], results[-2], results[-1]

    moved = []
    for p, (_, size) in enumerate(parts):
        held = results[1 + p * len(far) : 1 + (p + 1) * len(far)]
        moved.append([
            lax.ppermute(held[k - 2], "shard", [(s, s ^ k) for s in range(n)]).reshape(size * rows, width)
            for k in far
        ])

    ready_shape = jax.ShapeDtypeStruct((total, n * width), bf16)
    tall = max(r for r in range(16, PLACE_ROWS + 1, 16) if (done * rows) % r == 0 and (tail * rows) % r == 0)
    ready = pl.pallas_call(
        functools.partial(place_kernel, n, done * rows, tall),
        out_shape=ready_shape,
        in_specs=[hbm],
        out_specs=hbm,
        scratch_shapes=[pltpu.VMEM((RING, tall, width), bf16), dma((RING,)), dma((RING,))],
        compiler_params=pltpu.CompilerParams(vmem_limit_bytes=44 * 1024 * 1024),
        cost_estimate=pl.CostEstimate(flops=0, bytes_accessed=4 * done * n * rows * width, transcendentals=0),
        name="place_main",
    )(main)

    for (first, size), pieces in zip(parts, moved):
        ready = pl.pallas_call(
            functools.partial(finish_kernel, n, first * rows),
            out_shape=ready_shape,
            in_specs=[vmem] * len(far) + [hbm],
            out_specs=hbm,
            scratch_shapes=[dma((len(far),))],
            input_output_aliases={len(far): 0},
            compiler_params=pltpu.CompilerParams(vmem_limit_bytes=8 * 1024 * 1024),
            cost_estimate=pl.CostEstimate(
                flops=0, bytes_accessed=4 * size * len(far) * rows * width, transcendentals=0
            ),
            name="place_tail",
        )(*pieces, ready)

    position = lax.axis_index("shard").astype(jnp.int32)
    by_target = scales.reshape(experts, count // rows, n, rows)
    scale_down = lax.dynamic_index_in_dim(by_target, position, 2, keepdims=False).reshape(experts, count)
    serve_router = router.transpose(0, 2, 1, 3).reshape(ne * columns, n * depth).T
    return (ready.reshape(experts, count, n * width), scale_down, serve_router)


def solution(mesh):
    in_specs = (P("expert", None, "shard"), P("shard", "expert"), P("shard"))
    out_specs = (P("expert", "shard", None), P("expert", "shard"), P())
    return jax.shard_map(
        functools.partial(per_device, mesh.shape["shard"], mesh.shape["expert"]),
        mesh=mesh, in_specs=in_specs, out_specs=out_specs, check_vma=False,
    )
```

```python
import functools

import jax
import jax.numpy as jnp
from jax import lax
from jax.experimental import pallas as pl
from jax.experimental.pallas import tpu as pltpu
from jax.sharding import PartitionSpec as P

LANES = 128
LEAD = 16
HEAD = 4
AHEAD = 6
HOLD = 4
DEFER = 10
TAIL_PART = 8
PLACE_ROWS = 160
RING = 16
MESH = pl.DeviceIdType.MESH


def rows_per_step(count, n):
    fits = [r for r in range(16, count + 1, 16) if count % r == 0]
    return [r for r in fits if (n * r) % LANES == 0][0]


def swap(i, k):
    for b in range(k.bit_length()):
        if (k >> b) & 1:
            i = i + (1 << b) * (1 - 2 * ((i // (1 << b)) % 2))
    return i


def exchange_kernel(n, ne, rows, done, parts, lead, head, x_hbm, weight_ref, gain_ref, *rest):
    far = range(2, n)
    main_hbm = rest[0]
    tails = [rest[1 + p * len(far) : 1 + (p + 1) * len(far)] for p in range(len(parts))]
    rest = rest[1 + len(parts) * len(far) :]
    scale_ref, router_ref = rest[:2]
    (xbuf, narrow, own_max, direct_max, sib_max, chip_max, far_max, raw, raw_column, raw_narrow,
     load_sem, max_send, direct_recv, sib_recv, far_recv, data_send, data_recv, keep_sem,
     router_send, router_recv, raw_sem) = rest[2:]
    experts, all_rows, width = x_hbm.shape
    count = all_rows // n
    blocks = count // rows
    steps = experts * blocks
    slots = xbuf.shape[0]
    groups = n * rows // LANES
    me = lax.axis_index("shard")
    mine = lax.axis_index("expert")
    late = me % 2
    bits = [1 << b for b in range(ne.bit_length() - 1)]

    def load(i, t):
        e, b = i // blocks, i % blocks
        return pltpu.make_async_copy(
            x_hbm.at[e, pl.ds(t * count + b * rows, rows), :],
            xbuf.at[i % slots, pl.ds(t * rows, rows), :],
            load_sem.at[i % slots],
        )

    def start_load(i):
        for t in range(n):
            load(i, t).start()

    for i in range(min(AHEAD, steps)):
        start_load(i)

    barrier = pltpu.get_barrier_semaphore()
    for k in range(1, n):
        pl.semaphore_signal(barrier, inc=1, device_id={"shard": swap(me, k)}, device_id_type=MESH)
    for bit in bits:
        pl.semaphore_signal(barrier, inc=1, device_id={"expert": swap(mine, bit)}, device_id_type=MESH)

    router_ref[mine, me] = (weight_ref[...] * gain_ref[...]).astype(jnp.bfloat16)

    def local_max(i):
        @pl.when(i + AHEAD < steps)
        def _():
            start_load(i + AHEAD)

        slot = i % slots
        pltpu.make_async_copy(xbuf.at[slot], xbuf.at[slot], load_sem.at[slot]).wait()
        for g in range(groups):
            at = pl.ds(g * LANES, LANES)
            top = jnp.abs(xbuf[slot, at, 0:LANES])
            for c in range(LANES, width, LANES):
                top = jnp.maximum(top, jnp.abs(xbuf[slot, at, c : c + LANES]))
            own_max[i, :, at] = jnp.max(top.T, axis=0, keepdims=True)

    def max_copy(source, target, arrival, k):
        return pltpu.make_async_remote_copy(
            src_ref=source, dst_ref=target, send_sem=max_send.at[0], recv_sem=arrival,
            device_id={"shard": swap(me, k)}, device_id_type=MESH,
        )

    def send_direct(i):
        for k in range(1, n):
            max_copy(own_max.at[i], direct_max.at[i, k - 1], direct_recv.at[i], k).start()

    def send_sibling(i):
        max_copy(own_max.at[i], sib_max.at[i], sib_recv.at[i], 1).start()

    def join_sibling(i):
        pltpu.make_async_copy(sib_max.at[i], sib_max.at[i], sib_recv.at[i]).wait()
        chip_max[i] = jnp.maximum(own_max[i], sib_max[i])

    def send_far(i):
        for k in range(2, n, 2):
            max_copy(chip_max.at[i], far_max.at[i, k // 2 - 1], far_recv.at[i], k).start()

    def direct_full(j):
        pltpu.make_async_copy(direct_max.at[j], direct_max.at[j], direct_recv.at[j]).wait()
        full = own_max[j]
        for k in range(1, n):
            full = jnp.maximum(full, direct_max[j, k - 1])
        return full

    def staged_full(j):
        pltpu.make_async_copy(far_max.at[j], far_max.at[j], far_recv.at[j]).wait()
        full = chip_max[j]
        for k in range(2, n, 2):
            full = jnp.maximum(full, far_max[j, k // 2 - 1])
        return full

    def divide(j, full):
        slot = j % slots
        scale_ref[j] = full
        for g in range(groups):
            at = pl.ds(g * LANES, LANES)
            column = jnp.broadcast_to(full[:, g * LANES : (g + 1) * LANES], (LANES, LANES)).T
            for c in range(0, width, LANES):
                narrow[j, at, c : c + LANES] = (xbuf[slot, at, c : c + LANES] / column).astype(jnp.bfloat16)

    def block_of(j, k):
        return narrow.at[j, pl.ds(pl.multiple_of(swap(me, k) * rows, rows), rows), :]

    def spot(j, k):
        return main_hbm.at[k, pl.ds(pl.multiple_of(j * rows, rows), rows), :]

    def push(j, k):
        pltpu.make_async_remote_copy(
            src_ref=block_of(j, k),
            dst_ref=spot(j, k),
            send_sem=data_send.at[k],
            recv_sem=data_recv.at[k],
            device_id={"shard": swap(me, k)},
            device_id_type=MESH,
        ).start()

    def push_far(j):
        for k in reversed(far):
            i = j - late * (HOLD if k % 2 else HOLD + DEFER)

            @pl.when((i >= (1 if k == 2 else 0)) & (i < done))
            def _():
                push(i, k)

    def dispatch(j):
        push_far(j)
        if n > 1:
            push(j, 1)
        pltpu.make_async_copy(block_of(j, 0), spot(j, 0), keep_sem.at[0]).start()
        for p, (first, size) in enumerate(parts):
            @pl.when((j >= first) & (j < first + size))
            def _():
                for k in far:
                    pltpu.make_async_copy(block_of(j, k), tails[p][k - 2].at[j - first], keep_sem.at[1 + p]).start()

    def opening(j, carry):
        at = head + 2 * j
        local_max(at)
        local_max(at + 1)
        if not (isinstance(j, int) and j == 0):
            join_sibling(at - 2)
            join_sibling(at - 1)
        divide(j, direct_full(j) if isinstance(j, int) else staged_full(j))
        send_sibling(at)
        send_sibling(at + 1)
        if not (isinstance(j, int) and j == 0):
            send_far(at - 2)
            send_far(at - 1)
        dispatch(j)
        return carry

    def steady(j, carry):
        @pl.when(j + lead < steps)
        def _():
            local_max(j + lead)

        @pl.when(j + lead - 2 < steps)
        def _():
            join_sibling(j + lead - 2)

        divide(j, staged_full(j))

        @pl.when(j + lead < steps)
        def _():
            send_sibling(j + lead)

        @pl.when(j + lead - 2 < steps)
        def _():
            send_far(j + lead - 2)

        dispatch(j)
        return carry

    def raw_copy():
        return pltpu.make_async_remote_copy(
            src_ref=xbuf.at[0, pl.ds(pl.multiple_of(swap(me, 2) * rows, rows), rows), :],
            dst_ref=raw, send_sem=raw_sem.at[0], recv_sem=raw_sem.at[1],
            device_id={"shard": swap(me, 2)}, device_id_type=MESH,
        )

    def raw_finish():
        pltpu.make_async_copy(raw, raw, raw_sem.at[1]).wait()
        full = scale_ref[0]
        for g in range(groups):
            at = pl.ds(g * LANES, LANES)
            raw_column[at, :] = jnp.broadcast_to(full[:, g * LANES : (g + 1) * LANES], (LANES, LANES)).T
        column = raw_column[pl.ds(pl.multiple_of(me * rows, rows), rows), :]
        for c in range(0, width, LANES):
            raw_narrow[:, c : c + LANES] = (raw[:, c : c + LANES] / column).astype(jnp.bfloat16)

    for i in range(head):
        local_max(i)
    pl.semaphore_wait(barrier, n - 1 + len(bits))
    for i in range(head):
        send_direct(i)
    raw_copy().start()
    for k in range(1, n):
        pltpu.make_async_remote_copy(
            src_ref=router_ref.at[mine, me], dst_ref=router_ref.at[mine, me],
            send_sem=router_send.at[0], recv_sem=router_recv.at[0],
            device_id={"shard": swap(me, k)}, device_id_type=MESH,
        ).start()
    for j in range(head):
        opening(j, 0)
    pltpu.make_async_copy(raw, raw, raw_sem.at[0]).wait()
    lax.fori_loop(head, lead - head, opening, 0)

    pieces = router_ref.at[mine, 0 : n - 1]
    pltpu.make_async_copy(pieces, pieces, router_send.at[0]).wait()
    pltpu.make_async_copy(pieces, pieces, router_recv.at[0]).wait()
    for b, bit in enumerate(bits):
        held = router_ref.at[pl.ds(mine - mine % bit, bit)]
        pltpu.make_async_remote_copy(
            src_ref=held, dst_ref=held,
            send_sem=router_send.at[1 + b], recv_sem=router_recv.at[1 + b],
            device_id={"expert": swap(mine, bit)}, device_id_type=MESH,
        ).start()
        pltpu.make_async_copy(held, held, router_send.at[1 + b]).wait()
        pltpu.make_async_copy(held, held, router_recv.at[1 + b]).wait()

    raw_finish()
    lax.fori_loop(lead - head, steps, steady, 0)
    pltpu.make_async_copy(raw_narrow, spot(0, 2), keep_sem.at[0]).start()
    for j in range(steps, done + HOLD + DEFER):
        push_far(j)

    for _ in range(1, n):
        some = own_max.at[0:head]
        pltpu.make_async_copy(some, some, max_send.at[0]).wait()
    for _ in range(n // 2):
        some = own_max.at[head:steps]
        pltpu.make_async_copy(some, some, max_send.at[0]).wait()
    for p in range(len(parts)):
        for k in far:
            pltpu.make_async_copy(tails[p][k - 2], tails[p][k - 2], keep_sem.at[1 + p]).wait()
    every = narrow.at[0:steps, 0:rows, :]
    sent = narrow.at[0:done, 0:rows, :]
    scaled = narrow.at[0 : done - 1, 0:rows, :]
    pltpu.make_async_copy(every, every, keep_sem.at[0]).wait()
    pltpu.make_async_copy(raw_narrow, raw_narrow, keep_sem.at[0]).wait()
    for k in range(1, n):
        moved = every if k == 1 else scaled if k == 2 else sent
        pltpu.make_async_copy(moved, moved, data_send.at[k]).wait()
        pltpu.make_async_copy(moved, moved, data_recv.at[k]).wait()


def place_kernel(n, cut, tall, main_hbm, out_hbm, ring, load_sem, store_sem):
    total, width = main_hbm.shape[1:]
    me = lax.axis_index("shard")
    near = min(2, n)
    first = n * (cut // tall)
    chunks = first + near * ((total - cut) // tall)
    slots = ring.shape[0]
    behind = slots // 2

    def where(t):
        early = t < first
        u = t - first
        k = jnp.where(early, t % n, u % near)
        row = jnp.where(early, (t // n) * tall, cut + (u // near) * tall)
        source = 0
        for q in range(n):
            source = jnp.where(k == q, swap(me, q), source)
        return k, pl.multiple_of(row, tall), pl.multiple_of(source * width, LANES)

    def load(t):
        k, row, _ = where(t)
        return pltpu.make_async_copy(main_hbm.at[k, pl.ds(row, tall), :], ring.at[t % slots], load_sem.at[t % slots])

    def store(t):
        _, row, column = where(t)
        return pltpu.make_async_copy(
            ring.at[t % slots], out_hbm.at[pl.ds(row, tall), pl.ds(column, width)], store_sem.at[t % slots]
        )

    def step(t, carry):
        @pl.when((t >= slots) & (t < chunks + slots))
        def _():
            store(t - slots).wait()

        @pl.when(t < chunks)
        def _():
            load(t).start()

        @pl.when((t >= behind) & (t < chunks + behind))
        def _():
            load(t - behind).wait()
            store(t - behind).start()

        return carry

    lax.fori_loop(0, chunks + slots, step, 0)


def finish_kernel(n, row, *refs):
    count = n - 2
    parts, out_hbm, sem = refs[:count], refs[-2], refs[-1]
    me = lax.axis_index("shard")
    size, width = parts[0].shape

    def store(k):
        column = pl.multiple_of(swap(me, k) * width, LANES)
        return pltpu.make_async_copy(
            parts[k - 2], out_hbm.at[pl.ds(row, size), pl.ds(column, width)], sem.at[k - 2]
        )

    for k in range(2, n):
        store(k).start()
    for k in range(2, n):
        store(k).wait()


def per_device(n, ne, train_down, router_weight, router_gain):
    experts, all_rows, width = train_down.shape
    count = all_rows // n
    rows = rows_per_step(count, n)
    steps = experts * (count // rows)
    total = steps * rows
    lead = min(LEAD, steps // 2)
    head = min(HEAD, lead // 2)
    tail = max(2, steps // TAIL_PART)
    done = steps - tail
    last = max(1, tail // 5)
    parts = [(done, tail - last), (steps - last, last)]
    far = range(2, n)
    depth, columns = router_weight.shape
    rounds = ne.bit_length()
    bf16, f32 = jnp.bfloat16, jnp.float32
    hbm = pl.BlockSpec(memory_space=pl.ANY)
    vmem = pl.BlockSpec(memory_space=pltpu.VMEM)
    dma = pltpu.SemaphoreType.DMA
    results = pl.pallas_call(
        functools.partial(exchange_kernel, n, ne, rows, done, parts, lead, head),
        out_shape=[jax.ShapeDtypeStruct((n, total, width), bf16)]
        + [jax.ShapeDtypeStruct((size, rows, width), bf16) for _, size in parts for _ in far]
        + [
            jax.ShapeDtypeStruct((steps, 1, n * rows), f32),
            jax.ShapeDtypeStruct((ne, n, columns, depth), bf16),
        ],
        in_specs=[hbm, vmem, vmem],
        out_specs=[hbm] * (1 + len(parts) * len(far)) + [vmem, vmem],
        scratch_shapes=[
            pltpu.VMEM((lead + AHEAD + 1, n * rows, width), f32),
            pltpu.VMEM((steps, n * rows, width), bf16),
            pltpu.VMEM((steps, 1, n * rows), f32),
            pltpu.VMEM((head, n - 1, 1, n * rows), f32),
            pltpu.VMEM((steps, 1, n * rows), f32),
            pltpu.VMEM((steps, 1, n * rows), f32),
            pltpu.VMEM((steps, n // 2 - 1, 1, n * rows), f32),
            pltpu.VMEM((rows, width), f32),
            pltpu.VMEM((n * rows, LANES), f32),
            pltpu.VMEM((rows, width), bf16),
            dma((lead + AHEAD + 1,)),
            dma((1,)),
            dma((head,)),
            dma((steps,)),
            dma((steps,)),
            dma((n,)),
            dma((n,)),
            dma((1 + len(parts),)),
            dma((rounds,)),
            dma((rounds,)),
            dma((2,)),
        ],
        compiler_params=pltpu.CompilerParams(
            collective_id=0, has_side_effects=True, vmem_limit_bytes=60 * 1024 * 1024
        ),
        name="exchange",
    )(train_down, router_weight.T, router_gain[None, :])
    main, scales, router = results[0], results[-2], results[-1]

    moved = []
    for p, (_, size) in enumerate(parts):
        held = results[1 + p * len(far) : 1 + (p + 1) * len(far)]
        moved.append([
            lax.ppermute(held[k - 2], "shard", [(s, s ^ k) for s in range(n)]).reshape(size * rows, width)
            for k in far
        ])

    ready_shape = jax.ShapeDtypeStruct((total, n * width), bf16)
    tall = max(r for r in range(16, PLACE_ROWS + 1, 16) if (done * rows) % r == 0 and (tail * rows) % r == 0)
    ready = pl.pallas_call(
        functools.partial(place_kernel, n, done * rows, tall),
        out_shape=ready_shape,
        in_specs=[hbm],
        out_specs=hbm,
        scratch_shapes=[pltpu.VMEM((RING, tall, width), bf16), dma((RING,)), dma((RING,))],
        compiler_params=pltpu.CompilerParams(vmem_limit_bytes=44 * 1024 * 1024),
        cost_estimate=pl.CostEstimate(flops=0, bytes_accessed=4 * done * n * rows * width, transcendentals=0),
        name="place_main",
    )(main)

    for (first, size), pieces in zip(parts, moved):
        ready = pl.pallas_call(
            functools.partial(finish_kernel, n, first * rows),
            out_shape=ready_shape,
            in_specs=[vmem] * len(far) + [hbm],
            out_specs=hbm,
            scratch_shapes=[dma((len(far),))],
            input_output_aliases={len(far): 0},
            compiler_params=pltpu.CompilerParams(vmem_limit_bytes=8 * 1024 * 1024),
            cost_estimate=pl.CostEstimate(
                flops=0, bytes_accessed=4 * size * len(far) * rows * width, transcendentals=0
            ),
            name="place_tail",
        )(*pieces, ready)

    position = lax.axis_index("shard").astype(jnp.int32)
    by_target = scales.reshape(experts, count // rows, n, rows)
    scale_down = lax.dynamic_index_in_dim(by_target, position, 2, keepdims=False).reshape(experts, count)
    serve_router = router.transpose(0, 2, 1, 3).reshape(ne * columns, n * depth).T
    return (ready.reshape(experts, count, n * width), scale_down, serve_router)


def solution(mesh):
    in_specs = (P("expert", None, "shard"), P("shard", "expert"), P("shard"))
    out_specs = (P("expert", "shard", None), P("expert", "shard"), P())
    return jax.shard_map(
        functools.partial(per_device, mesh.shape["shard"], mesh.shape["expert"]),
        mesh=mesh, in_specs=in_specs, out_specs=out_specs, check_vma=False,
    )
```

```python
import functools

import jax
import jax.numpy as jnp
from jax import lax
from jax.experimental import pallas as pl
from jax.experimental.pallas import tpu as pltpu
from jax.sharding import PartitionSpec as P

LANES = 128
LEAD = 16
HEAD = 4
AHEAD = 6
HOLD = 4
DEFER = 10
TAIL_PART = 8
PLACE_ROWS = 160
RING = 16
MESH = pl.DeviceIdType.MESH


def rows_per_step(count, n):
    fits = [r for r in range(16, count + 1, 16) if count % r == 0]
    return [r for r in fits if (n * r) % LANES == 0][0]


def swap(i, k):
    for b in range(k.bit_length()):
        if (k >> b) & 1:
            i = i + (1 << b) * (1 - 2 * ((i // (1 << b)) % 2))
    return i


def exchange_kernel(n, ne, rows, done, parts, lead, head, x_hbm, weight_hbm, gain_hbm, *rest):
    far = range(2, n)
    main_hbm = rest[0]
    tails = [rest[1 + p * len(far) : 1 + (p + 1) * len(far)] for p in range(len(parts))]
    rest = rest[1 + len(parts) * len(far) :]
    scale_ref, router_ref = rest[:2]
    (xbuf, narrow, own_max, direct_max, sib_max, chip_max, far_max, raw, raw_column, raw_narrow,
     load_sem, max_send, direct_recv, sib_recv, far_recv, data_send, data_recv, keep_sem,
     router_send, router_recv, raw_sem, weight, gain, weight_sem) = rest[2:]
    experts, all_rows, width = x_hbm.shape
    count = all_rows // n
    blocks = count // rows
    steps = experts * blocks
    slots = xbuf.shape[0]
    groups = n * rows // LANES
    me = lax.axis_index("shard")
    mine = lax.axis_index("expert")
    late = me % 2
    bits = [1 << b for b in range(ne.bit_length() - 1)]

    def load(i, t):
        e, b = i // blocks, i % blocks
        return pltpu.make_async_copy(
            x_hbm.at[e, pl.ds(t * count + b * rows, rows), :],
            xbuf.at[i % slots, pl.ds(t * rows, rows), :],
            load_sem.at[i % slots],
        )

    def start_load(i):
        for t in range(n):
            load(i, t).start()

    for i in range(min(AHEAD, steps)):
        start_load(i)

    barrier = pltpu.get_barrier_semaphore()
    for k in range(1, n):
        pl.semaphore_signal(barrier, inc=1, device_id={"shard": swap(me, k)}, device_id_type=MESH)
    for bit in bits:
        pl.semaphore_signal(barrier, inc=1, device_id={"expert": swap(mine, bit)}, device_id_type=MESH)

    fetch = [
        pltpu.make_async_copy(weight_hbm, weight, weight_sem.at[0]),
        pltpu.make_async_copy(gain_hbm, gain, weight_sem.at[1]),
    ]
    for copy in fetch:
        copy.start()

    def local_max(i):
        @pl.when(i + AHEAD < steps)
        def _():
            start_load(i + AHEAD)

        slot = i % slots
        pltpu.make_async_copy(xbuf.at[slot], xbuf.at[slot], load_sem.at[slot]).wait()
        for g in range(groups):
            at = pl.ds(g * LANES, LANES)
            top = jnp.abs(xbuf[slot, at, 0:LANES])
            for c in range(LANES, width, LANES):
                top = jnp.maximum(top, jnp.abs(xbuf[slot, at, c : c + LANES]))
            own_max[i, :, at] = jnp.max(top.T, axis=0, keepdims=True)

    def max_copy(source, target, arrival, k):
        return pltpu.make_async_remote_copy(
            src_ref=source, dst_ref=target, send_sem=max_send.at[0], recv_sem=arrival,
            device_id={"shard": swap(me, k)}, device_id_type=MESH,
        )

    def send_direct(i):
        for k in range(1, n):
            max_copy(own_max.at[i], direct_max.at[i, k - 1], direct_recv.at[i], k).start()

    def send_sibling(i):
        max_copy(own_max.at[i], sib_max.at[i], sib_recv.at[i], 1).start()

    def join_sibling(i):
        pltpu.make_async_copy(sib_max.at[i], sib_max.at[i], sib_recv.at[i]).wait()
        chip_max[i] = jnp.maximum(own_max[i], sib_max[i])

    def send_far(i):
        for k in range(2, n, 2):
            max_copy(chip_max.at[i], far_max.at[i, k // 2 - 1], far_recv.at[i], k).start()

    def direct_full(j):
        pltpu.make_async_copy(direct_max.at[j], direct_max.at[j], direct_recv.at[j]).wait()
        full = own_max[j]
        for k in range(1, n):
            full = jnp.maximum(full, direct_max[j, k - 1])
        return full

    def staged_full(j):
        pltpu.make_async_copy(far_max.at[j], far_max.at[j], far_recv.at[j]).wait()
        full = chip_max[j]
        for k in range(2, n, 2):
            full = jnp.maximum(full, far_max[j, k // 2 - 1])
        return full

    def divide(j, full):
        slot = j % slots
        scale_ref[j] = full
        for g in range(groups):
            at = pl.ds(g * LANES, LANES)
            column = jnp.broadcast_to(full[:, g * LANES : (g + 1) * LANES], (LANES, LANES)).T
            for c in range(0, width, LANES):
                narrow[j, at, c : c + LANES] = (xbuf[slot, at, c : c + LANES] / column).astype(jnp.bfloat16)

    def block_of(j, k):
        return narrow.at[j, pl.ds(pl.multiple_of(swap(me, k) * rows, rows), rows), :]

    def spot(j, k):
        return main_hbm.at[k, pl.ds(pl.multiple_of(j * rows, rows), rows), :]

    def push(j, k):
        pltpu.make_async_remote_copy(
            src_ref=block_of(j, k),
            dst_ref=spot(j, k),
            send_sem=data_send.at[k],
            recv_sem=data_recv.at[k],
            device_id={"shard": swap(me, k)},
            device_id_type=MESH,
        ).start()

    def push_far(j):
        for k in reversed(far):
            i = j - late * (HOLD if k % 2 else HOLD + DEFER)

            @pl.when((i >= (1 if k == 2 else 0)) & (i < done))
            def _():
                push(i, k)

    def dispatch(j):
        push_far(j)
        if n > 1:
            push(j, 1)
        pltpu.make_async_copy(block_of(j, 0), spot(j, 0), keep_sem.at[0]).start()
        for p, (first, size) in enumerate(parts):
            @pl.when((j >= first) & (j < first + size))
            def _():
                for k in far:
                    pltpu.make_async_copy(block_of(j, k), tails[p][k - 2].at[j - first], keep_sem.at[1 + p]).start()

    def opening(j, carry):
        at = head + 2 * j
        local_max(at)
        local_max(at + 1)
        if not (isinstance(j, int) and j == 0):
            join_sibling(at - 2)
            join_sibling(at - 1)
        divide(j, direct_full(j) if isinstance(j, int) else staged_full(j))
        send_sibling(at)
        send_sibling(at + 1)
        if not (isinstance(j, int) and j == 0):
            send_far(at - 2)
            send_far(at - 1)
        dispatch(j)
        return carry

    def steady(j, carry):
        @pl.when(j + lead < steps)
        def _():
            local_max(j + lead)

        @pl.when(j + lead - 2 < steps)
        def _():
            join_sibling(j + lead - 2)

        divide(j, staged_full(j))

        @pl.when(j + lead < steps)
        def _():
            send_sibling(j + lead)

        @pl.when(j + lead - 2 < steps)
        def _():
            send_far(j + lead - 2)

        dispatch(j)
        return carry

    def raw_copy():
        return pltpu.make_async_remote_copy(
            src_ref=xbuf.at[0, pl.ds(pl.multiple_of(swap(me, 2) * rows, rows), rows), :],
            dst_ref=raw, send_sem=raw_sem.at[0], recv_sem=raw_sem.at[1],
            device_id={"shard": swap(me, 2)}, device_id_type=MESH,
        )

    def raw_finish():
        pltpu.make_async_copy(raw, raw, raw_sem.at[1]).wait()
        full = scale_ref[0]
        for g in range(groups):
            at = pl.ds(g * LANES, LANES)
            raw_column[at, :] = jnp.broadcast_to(full[:, g * LANES : (g + 1) * LANES], (LANES, LANES)).T
        column = raw_column[pl.ds(pl.multiple_of(me * rows, rows), rows), :]
        for c in range(0, width, LANES):
            raw_narrow[:, c : c + LANES] = (raw[:, c : c + LANES] / column).astype(jnp.bfloat16)

    for i in range(head):
        local_max(i)
    for copy in fetch:
        copy.wait()
    router_ref[mine, me] = (weight[...] * gain[...]).astype(jnp.bfloat16)
    pl.semaphore_wait(barrier, n - 1 + len(bits))
    for i in range(head):
        send_direct(i)
    raw_copy().start()
    for k in range(1, n):
        pltpu.make_async_remote_copy(
            src_ref=router_ref.at[mine, me], dst_ref=router_ref.at[mine, me],
            send_sem=router_send.at[0], recv_sem=router_recv.at[0],
            device_id={"shard": swap(me, k)}, device_id_type=MESH,
        ).start()
    for j in range(head):
        opening(j, 0)
    pltpu.make_async_copy(raw, raw, raw_sem.at[0]).wait()
    lax.fori_loop(head, lead - head, opening, 0)

    pieces = router_ref.at[mine, 0 : n - 1]
    pltpu.make_async_copy(pieces, pieces, router_send.at[0]).wait()
    pltpu.make_async_copy(pieces, pieces, router_recv.at[0]).wait()
    for b, bit in enumerate(bits):
        held = router_ref.at[pl.ds(mine - mine % bit, bit)]
        pltpu.make_async_remote_copy(
            src_ref=held, dst_ref=held,
            send_sem=router_send.at[1 + b], recv_sem=router_recv.at[1 + b],
            device_id={"expert": swap(mine, bit)}, device_id_type=MESH,
        ).start()
        pltpu.make_async_copy(held, held, router_send.at[1 + b]).wait()
        pltpu.make_async_copy(held, held, router_recv.at[1 + b]).wait()

    raw_finish()
    lax.fori_loop(lead - head, steps, steady, 0)
    pltpu.make_async_copy(raw_narrow, spot(0, 2), keep_sem.at[0]).start()
    for j in range(steps, done + HOLD + DEFER):
        push_far(j)

    for _ in range(1, n):
        some = own_max.at[0:head]
        pltpu.make_async_copy(some, some, max_send.at[0]).wait()
    for _ in range(n // 2):
        some = own_max.at[head:steps]
        pltpu.make_async_copy(some, some, max_send.at[0]).wait()
    for p in range(len(parts)):
        for k in far:
            pltpu.make_async_copy(tails[p][k - 2], tails[p][k - 2], keep_sem.at[1 + p]).wait()
    every = narrow.at[0:steps, 0:rows, :]
    sent = narrow.at[0:done, 0:rows, :]
    scaled = narrow.at[0 : done - 1, 0:rows, :]
    pltpu.make_async_copy(every, every, keep_sem.at[0]).wait()
    pltpu.make_async_copy(raw_narrow, raw_narrow, keep_sem.at[0]).wait()
    for k in range(1, n):
        moved = every if k == 1 else scaled if k == 2 else sent
        pltpu.make_async_copy(moved, moved, data_send.at[k]).wait()
        pltpu.make_async_copy(moved, moved, data_recv.at[k]).wait()


def place_kernel(n, cut, tall, main_hbm, out_hbm, ring, load_sem, store_sem):
    total, width = main_hbm.shape[1:]
    me = lax.axis_index("shard")
    near = min(2, n)
    first = n * (cut // tall)
    chunks = first + near * ((total - cut) // tall)
    slots = ring.shape[0]
    behind = slots // 2

    def where(t):
        early = t < first
        u = t - first
        k = jnp.where(early, t % n, u % near)
        row = jnp.where(early, (t // n) * tall, cut + (u // near) * tall)
        source = 0
        for q in range(n):
            source = jnp.where(k == q, swap(me, q), source)
        return k, pl.multiple_of(row, tall), pl.multiple_of(source * width, LANES)

    def load(t):
        k, row, _ = where(t)
        return pltpu.make_async_copy(main_hbm.at[k, pl.ds(row, tall), :], ring.at[t % slots], load_sem.at[t % slots])

    def store(t):
        _, row, column = where(t)
        return pltpu.make_async_copy(
            ring.at[t % slots], out_hbm.at[pl.ds(row, tall), pl.ds(column, width)], store_sem.at[t % slots]
        )

    def step(t, carry):
        @pl.when((t >= slots) & (t < chunks + slots))
        def _():
            store(t - slots).wait()

        @pl.when(t < chunks)
        def _():
            load(t).start()

        @pl.when((t >= behind) & (t < chunks + behind))
        def _():
            load(t - behind).wait()
            store(t - behind).start()

        return carry

    lax.fori_loop(0, chunks + slots, step, 0)


def finish_kernel(n, row, *refs):
    count = n - 2
    parts, out_hbm, sem = refs[:count], refs[-2], refs[-1]
    me = lax.axis_index("shard")
    size, width = parts[0].shape

    def store(k):
        column = pl.multiple_of(swap(me, k) * width, LANES)
        return pltpu.make_async_copy(
            parts[k - 2], out_hbm.at[pl.ds(row, size), pl.ds(column, width)], sem.at[k - 2]
        )

    for k in range(2, n):
        store(k).start()
    for k in range(2, n):
        store(k).wait()


def per_device(n, ne, train_down, router_weight, router_gain):
    experts, all_rows, width = train_down.shape
    count = all_rows // n
    rows = rows_per_step(count, n)
    steps = experts * (count // rows)
    total = steps * rows
    lead = min(LEAD, steps // 2)
    head = min(HEAD, lead // 2)
    tail = max(2, steps // TAIL_PART)
    done = steps - tail
    last = max(1, tail // 5)
    parts = [(done, tail - last), (steps - last, last)]
    far = range(2, n)
    depth, columns = router_weight.shape
    rounds = ne.bit_length()
    bf16, f32 = jnp.bfloat16, jnp.float32
    hbm = pl.BlockSpec(memory_space=pl.ANY)
    vmem = pl.BlockSpec(memory_space=pltpu.VMEM)
    dma = pltpu.SemaphoreType.DMA
    results = pl.pallas_call(
        functools.partial(exchange_kernel, n, ne, rows, done, parts, lead, head),
        out_shape=[jax.ShapeDtypeStruct((n, total, width), bf16)]
        + [jax.ShapeDtypeStruct((size, rows, width), bf16) for _, size in parts for _ in far]
        + [
            jax.ShapeDtypeStruct((steps, 1, n * rows), f32),
            jax.ShapeDtypeStruct((ne, n, columns, depth), bf16),
        ],
        in_specs=[hbm, hbm, hbm],
        out_specs=[hbm] * (1 + len(parts) * len(far)) + [vmem, vmem],
        scratch_shapes=[
            pltpu.VMEM((lead + AHEAD + 1, n * rows, width), f32),
            pltpu.VMEM((steps, n * rows, width), bf16),
            pltpu.VMEM((steps, 1, n * rows), f32),
            pltpu.VMEM((head, n - 1, 1, n * rows), f32),
            pltpu.VMEM((steps, 1, n * rows), f32),
            pltpu.VMEM((steps, 1, n * rows), f32),
            pltpu.VMEM((steps, n // 2 - 1, 1, n * rows), f32),
            pltpu.VMEM((rows, width), f32),
            pltpu.VMEM((n * rows, LANES), f32),
            pltpu.VMEM((rows, width), bf16),
            dma((lead + AHEAD + 1,)),
            dma((1,)),
            dma((head,)),
            dma((steps,)),
            dma((steps,)),
            dma((n,)),
            dma((n,)),
            dma((1 + len(parts),)),
            dma((rounds,)),
            dma((rounds,)),
            dma((2,)),
            pltpu.VMEM((columns, depth), f32),
            pltpu.VMEM((1, depth), f32),
            dma((2,)),
        ],
        compiler_params=pltpu.CompilerParams(
            collective_id=0, has_side_effects=True, vmem_limit_bytes=60 * 1024 * 1024
        ),
        name="exchange",
    )(train_down, router_weight.T, router_gain[None, :])
    main, scales, router = results[0], results[-2], results[-1]

    moved = []
    for p, (_, size) in enumerate(parts):
        held = results[1 + p * len(far) : 1 + (p + 1) * len(far)]
        moved.append([
            lax.ppermute(held[k - 2], "shard", [(s, s ^ k) for s in range(n)]).reshape(size * rows, width)
            for k in far
        ])

    ready_shape = jax.ShapeDtypeStruct((total, n * width), bf16)
    tall = max(r for r in range(16, PLACE_ROWS + 1, 16) if (done * rows) % r == 0 and (tail * rows) % r == 0)
    ready = pl.pallas_call(
        functools.partial(place_kernel, n, done * rows, tall),
        out_shape=ready_shape,
        in_specs=[hbm],
        out_specs=hbm,
        scratch_shapes=[pltpu.VMEM((RING, tall, width), bf16), dma((RING,)), dma((RING,))],
        compiler_params=pltpu.CompilerParams(vmem_limit_bytes=44 * 1024 * 1024),
        cost_estimate=pl.CostEstimate(flops=0, bytes_accessed=4 * done * n * rows * width, transcendentals=0),
        name="place_main",
    )(main)

    for (first, size), pieces in zip(parts, moved):
        ready = pl.pallas_call(
            functools.partial(finish_kernel, n, first * rows),
            out_shape=ready_shape,
            in_specs=[vmem] * len(far) + [hbm],
            out_specs=hbm,
            scratch_shapes=[dma((len(far),))],
            input_output_aliases={len(far): 0},
            compiler_params=pltpu.CompilerParams(vmem_limit_bytes=8 * 1024 * 1024),
            cost_estimate=pl.CostEstimate(
                flops=0, bytes_accessed=4 * size * len(far) * rows * width, transcendentals=0
            ),
            name="place_tail",
        )(*pieces, ready)

    position = lax.axis_index("shard").astype(jnp.int32)
    by_target = scales.reshape(experts, count // rows, n, rows)
    scale_down = lax.dynamic_index_in_dim(by_target, position, 2, keepdims=False).reshape(experts, count)
    serve_router = router.transpose(0, 2, 1, 3).reshape(ne * columns, n * depth).T
    return (ready.reshape(experts, count, n * width), scale_down, serve_router)


def solution(mesh):
    in_specs = (P("expert", None, "shard"), P("shard", "expert"), P("shard"))
    out_specs = (P("expert", "shard", None), P("expert", "shard"), P())
    return jax.shard_map(
        functools.partial(per_device, mesh.shape["shard"], mesh.shape["expert"]),
        mesh=mesh, in_specs=in_specs, out_specs=out_specs, check_vma=False,
    )
```
